32 devices in a mesh: gx: 2 (over y), gy: 4 (over z), gz: 4 (over x, core).
Axes of the slice: x: 2, y: 2, z: 4, core: 2. Of those that a mesh axis runs over, the one named last changes fastest.
Arguments:
- source: float32 [2, 8, 32, 512], P(None, 'gx', 'gy', 'gz'), may hold values from -6 to 6
- sigma_intra: float32 [3, 8, 32, 512], P(None, 'gx', 'gy', 'gz'), may hold values from 0.3 to 3
- sigma_extra: float32 [3, 8, 32, 512], P(None, 'gx', 'gy', 'gz'), may hold values from 0.5 to 3
- membrane: float32 [8, 32, 512], P('gx', 'gy', 'gz'), may hold values from 0.5 to 5
Outputs:
- solution: float32 [2, 8, 32, 512], P(None, 'gx', 'gy', 'gz')
- residual: float32 [2, 8, 32, 512], P(None, 'gx', 'gy', 'gz')
The draws below stay inside these ranges and needn't reach their ends.
All inputs are finite; a program needn't handle non-finite values.
Results may differ from the reference program's by a relative error of at most 0.0009.
Values sent between devices are 32-bit elements; how exact they have to be, the bound alone decides.
A program may use at most 64 MiB of HBM per device.

```python
import math
import jax
import jax.numpy as jnp
from jax import lax

KRYLOV = 10
NX = 8
NY = 32
NZ = 512


def steps_of(stream_key, shape, shards, low, largest):
    gain, own = 1.0, jax.random.fold_in(stream_key, 6)
    for dim, parts in shards:
        draws = jnp.exp(jax.random.uniform(jax.random.fold_in(own, dim), (parts,), jnp.float32, low / len(shards), largest / len(shards)))
        gain = gain * jnp.repeat(draws, shape[dim] // parts).reshape([-1 if axis == dim else 1 for axis in range(len(shape))])
    return gain


def normal_values(stream_key, shape, width, most, shards=(), dtype=jnp.bfloat16):
    array = jax.random.normal(stream_key, shape, jnp.float32) * width
    if len(shards) > 0:
        array = steps_of(stream_key, shape, shards, -0.22, 0.18) * array
    return jnp.clip(array, min=-most, max=most).astype(dtype)


def setup_inputs(seed: int = 0) -> dict:
    keys = jax.random.split(jax.random.key(seed), 5)
    return {
        "source": normal_values(keys[0], (2, NX, NY, NZ), 1.0, 6.0, ((1, 2), (2, 4), (3, 4)), jnp.float32),
        "sigma_intra": jnp.clip(jnp.exp(math.log(3.0) - 2.3025851 * jax.random.uniform(keys[1], (3, NX, NY, NZ), jnp.float32) ** steps_of(keys[1], (3, NX, NY, NZ), ((1, 2), (2, 4), (3, 4)), -0.2, 0.2)), 0.3, 3.0),
        "sigma_extra": jnp.clip(jnp.exp(math.log(3.0) - 1.7917595 * jax.random.uniform(keys[2], (3, NX, NY, NZ), jnp.float32) ** steps_of(keys[2], (3, NX, NY, NZ), ((1, 2), (2, 4), (3, 4)), -0.2, 0.2)), 0.5, 3.0),
        "membrane": jnp.clip(jnp.exp(math.log(5.0) - 2.3025851 * jax.random.uniform(keys[3], (NX, NY, NZ), jnp.float32) ** steps_of(keys[3], (NX, NY, NZ), ((0, 2), (1, 4), (2, 4)), -0.2, 0.2)), 0.5, 5.0),
    }


highest = lax.Precision.HIGHEST

def shifted(padded_grid, spatial, offset):
    pieces = [slice(1, -1), slice(1, -1), slice(1, -1)]
    if offset > 0:
        pieces[spatial] = slice(2, None)
    else:
        pieces[spatial] = slice(None, -2)
    return padded_grid[tuple(pieces)]

def face_terms(padded_sigma):
    upper_faces = []
    lower_faces = []
    for spatial in range(3):
        component = padded_sigma[spatial]
        middle = component[1:-1, 1:-1, 1:-1]
        upper_faces.append(0.5 * (middle + shifted(component, spatial, 1)))
        lower_faces.append(0.5 * (middle + shifted(component, spatial, -1)))
    diagonal = upper_faces[0] + lower_faces[0]
    for spatial in range(1, 3):
        diagonal = diagonal + upper_faces[spatial] + lower_faces[spatial]
    return (upper_faces, lower_faces, diagonal)

def apply_laplace(faces, padded_field):
    upper_faces, lower_faces, diagonal = faces
    result = diagonal * padded_field[1:-1, 1:-1, 1:-1]
    for spatial in range(3):
        result = result - upper_faces[spatial] * shifted(padded_field, spatial, 1)
        result = result - lower_faces[spatial] * shifted(padded_field, spatial, -1)
    return result

def operate(intra_faces, extra_faces, membrane, padded_pair):
    joined = padded_pair[0] + padded_pair[1]
    shared = apply_laplace(intra_faces, joined)
    leading = membrane * padded_pair[0, 1:-1, 1:-1, 1:-1] + shared
    second = shared + apply_laplace(extra_faces, padded_pair[1])
    return jnp.stack([leading, second])

def inverse_blocks(intra_faces, extra_faces, membrane):
    intra_sum = intra_faces[2]
    extra_sum = extra_faces[2]
    determinant = membrane * intra_sum + membrane * extra_sum + intra_sum * extra_sum
    return jnp.stack([(intra_sum + extra_sum) / determinant, -intra_sum / determinant, (membrane + intra_sum) / determinant])

def precondition(inverse, pair):
    leading = inverse[0] * pair[0] + inverse[1] * pair[1]
    second = inverse[1] * pair[0] + inverse[2] * pair[1]
    return jnp.stack([leading, second])

def least_squares(hessenberg, start_norm):
    krylov = hessenberg.shape[1]
    rotated = hessenberg
    target = jnp.zeros((krylov + 1,), jnp.float32).at[0].set(start_norm)
    for column in range(krylov):
        pivot = rotated[column, column]
        lower_entry = rotated[column + 1, column]
        radius = jnp.sqrt(pivot * pivot + lower_entry * lower_entry)
        cosine = pivot / radius
        sine_value = lower_entry / radius
        row_top = cosine * rotated[column] + sine_value * rotated[column + 1]
        row_below = -sine_value * rotated[column] + cosine * rotated[column + 1]
        rotated = rotated.at[column].set(row_top).at[column + 1].set(row_below)
        leading = cosine * target[column] + sine_value * target[column + 1]
        second = -sine_value * target[column] + cosine * target[column + 1]
        target = target.at[column].set(leading).at[column + 1].set(second)
    coeffs = jnp.zeros((krylov,), jnp.float32)
    for column in range(krylov - 1, -1, -1):
        partial_sum = jnp.sum(rotated[column, column + 1:] * coeffs[column + 1:])
        coeffs = coeffs.at[column].set((target[column] - partial_sum) / rotated[column, column])
    return coeffs

def reference(source, sigma_intra, sigma_extra, membrane):
    margins = ((0, 0), (1, 1), (1, 1), (1, 1))
    intra_faces = face_terms(jnp.pad(sigma_intra, margins))
    extra_faces = face_terms(jnp.pad(sigma_extra, margins))
    inverse = inverse_blocks(intra_faces, extra_faces, membrane)
    start_norm = jnp.sqrt(jnp.sum(source * source))
    basis = jnp.zeros((KRYLOV + 1,) + source.shape, jnp.float32).at[0].set(source / start_norm)
    hessenberg = jnp.zeros((KRYLOV + 1, KRYLOV), jnp.float32)
    for column in range(KRYLOV):
        solved = precondition(inverse, basis[column])
        applied = operate(intra_faces, extra_faces, membrane, jnp.pad(solved, margins))
        flat_basis = basis[:column + 1].reshape(column + 1, -1)
        project = jnp.dot(flat_basis, applied.reshape(-1), precision=highest)
        applied = applied - jnp.dot(project, flat_basis, precision=highest).reshape(applied.shape)
        new_norm = jnp.sqrt(jnp.sum(applied * applied))
        basis = basis.at[column + 1].set(applied / new_norm)
        hessenberg = hessenberg.at[:column + 1, column].set(project).at[column + 1, column].set(new_norm)
    coeffs = least_squares(hessenberg, start_norm)
    combined = jnp.dot(coeffs, basis[:KRYLOV].reshape(KRYLOV, -1), precision=highest).reshape(source.shape)
    solution = precondition(inverse, combined)
    remainder = jnp.zeros((KRYLOV + 1,), jnp.float32).at[0].set(start_norm) - jnp.dot(hessenberg, coeffs, precision=highest)
    residual = jnp.dot(remainder, basis.reshape(KRYLOV + 1, -1), precision=highest).reshape(source.shape)
    return (solution, residual)
```

```python
import functools
import math

import jax
import jax.numpy as jnp
from jax import lax
from jax.experimental import pallas as pl
from jax.experimental.pallas import tpu as pltpu
from jax.sharding import PartitionSpec as P

KRYLOV = 10
FIRST = 5
SCALE = 0.9
AXES = ("gx", "gy", "gz")
MESH = pl.DeviceIdType.MESH
highest = lax.Precision.HIGHEST

TAU = [math.cosh(k * math.acosh(1.0 / SCALE)) for k in range(KRYLOV + 1)]


def cholesky(matrix, count):
    lower = {}
    inverse_diag = []
    for j in range(count):
        pivot = matrix[j, j]
        for m in range(j):
            pivot = pivot - lower[j, m] * lower[j, m]
        inverse_root = lax.rsqrt(pivot)
        inverse_root = inverse_root * (1.5 - 0.5 * pivot * inverse_root * inverse_root)
        inverse_diag.append(inverse_root)
        for i in range(j + 1, count):
            value = matrix[i, j]
            for m in range(j):
                value = value - lower[i, m] * lower[j, m]
            lower[i, j] = value * inverse_root
    return lower, inverse_diag


def forward_solve(lower, inverse_diag, rhs):
    out = []
    for i in range(len(rhs)):
        value = rhs[i]
        for m in range(i):
            value = value - lower[i, m] * out[m]
        out.append(value * inverse_diag[i])
    return out


def backward_solve(lower, inverse_diag, rhs):
    count = len(rhs)
    out = [None] * count
    for i in range(count - 1, -1, -1):
        value = rhs[i]
        for m in range(i + 1, count):
            value = value - lower[m, i] * out[m]
        out[i] = value * inverse_diag[i]
    return out


def kernel(
    sizes,
    source,
    intra,
    extra,
    membrane,
    solution_ref,
    residual_ref,
    basis,
    faces_x,
    faces_y,
    faces_z,
    inverse,
    field,
    pack_y,
    pack_z,
    halo_x,
    halo_y,
    halo_z,
    gram,
    parts,
    send_sem,
    recv_sem,
    sum_send,
    sum_recv,
):
    planes, rows, lanes = source.shape[1:]
    total = 2 * planes
    place = [lax.axis_index(axis) for axis in AXES]
    lane = lax.broadcasted_iota(jnp.int32, (rows, lanes), 1)
    row = lax.broadcasted_iota(jnp.int32, (rows, lanes), 0)

    def edge_conditions(dim):
        return (place[dim] > 0, place[dim] < sizes[dim] - 1)

    halos = (halo_x, halo_y, halo_z)

    def send_source(dim, slot, side):
        if dim == 0:
            return field.at[slot, :, planes - 1 if side == 1 else 0]
        if dim == 1:
            return pack_y.at[slot, side]
        return pack_z.at[slot]

    def copy_to(dim, slot, side):
        return pltpu.make_async_remote_copy(
            src_ref=send_source(dim, slot, side),
            dst_ref=halos[dim].at[slot, 1 - side],
            send_sem=send_sem.at[slot, dim, side],
            recv_sem=recv_sem.at[slot, dim, 1 - side],
            device_id={AXES[dim]: place[dim] + (1 if side == 1 else -1)},
            device_id_type=MESH,
        )

    def copy_from(dim, slot, side):
        return pltpu.make_async_remote_copy(
            src_ref=send_source(dim, slot, side),
            dst_ref=halos[dim].at[slot, side],
            send_sem=send_sem.at[slot, dim, side],
            recv_sem=recv_sem.at[slot, dim, side],
            device_id={AXES[dim]: place[dim] + (1 if side == 1 else -1)},
            device_id_type=MESH,
        )

    def each_neighbour(action):
        for dim in (2, 1, 0):
            for side in range(2):
                pl.when(edge_conditions(dim)[side])(functools.partial(action, dim, side))

    def start(slot):
        each_neighbour(lambda dim, side: copy_to(dim, slot, side).start())

    def finish(slot):
        each_neighbour(lambda dim, side: copy_from(dim, slot, side).wait_recv())

    def drain(slot):
        each_neighbour(lambda dim, side: copy_to(dim, slot, side).wait_send())

    def set_packs(slot, values_y, values_z):
        pack_y[slot, 0] = jnp.concatenate([v[0:1] for v in values_y], axis=0)
        pack_y[slot, 1] = jnp.concatenate([v[rows - 1 : rows] for v in values_y], axis=0)
        edges = jnp.zeros((rows, lanes), jnp.float32)
        for k, value in enumerate(values_z):
            turned = pltpu.roll(value, 2 * k + 1, 1)
            edges = jnp.where((lane == 2 * k) | (lane == 2 * k + 1), turned, edges)
        pack_z[slot] = edges

    def zero_edges(dim, side):
        halos[dim][:, side] = jnp.zeros(halos[dim].shape[:1] + halos[dim].shape[2:], jnp.float32)

    for dim in range(3):
        for side in range(2):
            outside = place[dim] == (0 if side == 0 else sizes[dim] - 1)
            pl.when(outside)(functools.partial(zero_edges, dim, side))

    def halo_up_z(slot, k):
        return pltpu.roll(halo_z[slot, 1], lanes - 2 - 2 * k, 1)

    def halo_down_z(slot, k):
        return pltpu.roll(halo_z[slot, 0], (lanes - 2 * k) % lanes, 1)

    def halo_y_row(slot, side, k):
        return jnp.broadcast_to(halo_y[slot, side, k : k + 1, :], (rows, lanes))

    sigma = (intra, extra)
    for c in range(2):
        for x in (0, planes - 1):
            field[0, c, x] = sigma[c][0, x]
    order = [(c, x) for c in range(2) for x in range(planes)]
    set_packs(0, [sigma[c][1, x] for c, x in order], [sigma[c][2, x] for c, x in order])
    start(0)
    gram[...] = jnp.zeros_like(gram)
    for k, (c, x) in enumerate(order):
        basis[0, k] = source[c, x]
    finish(0)
    factor = 1.0 / SCALE
    diagonals = []
    for k, (c, x) in enumerate(order):
        mine = sigma[c][0, x]
        above = sigma[c][0, x + 1] if x < planes - 1 else halo_x[0, 1, c]
        below = sigma[c][0, x - 1] if x > 0 else halo_x[0, 0, c]
        up, down = mine + above, mine + below
        diagonal = up + down
        faces_x[0, k] = factor * up
        faces_x[1, k] = factor * down
        mine = sigma[c][1, x]
        above = jnp.where(row < rows - 1, pltpu.roll(mine, rows - 1, 0), halo_y_row(0, 1, k))
        below = jnp.where(row > 0, pltpu.roll(mine, 1, 0), halo_y_row(0, 0, k))
        up, down = mine + above, mine + below
        diagonal = diagonal + up + down
        up, down = factor * up, factor * down
        faces_y[0, k] = jnp.where(row < rows - 1, up, 0.0)
        faces_y[1, k] = jnp.where(row > 0, down, 0.0)
        faces_y[2, k] = jnp.where(row < rows - 1, 0.0, up)
        faces_y[3, k] = jnp.where(row > 0, 0.0, down)
        mine = sigma[c][2, x]
        above = jnp.where(lane < lanes - 1, pltpu.roll(mine, lanes - 1, 1), halo_up_z(0, k))
        below = jnp.where(lane > 0, pltpu.roll(mine, 1, 1), halo_down_z(0, k))
        up, down = mine + above, mine + below
        diagonal = diagonal + up + down
        up, down = factor * up, factor * down
        faces_z[0, k] = jnp.where(lane < lanes - 1, up, 0.0)
        faces_z[1, k] = jnp.where(lane > 0, down, 0.0)
        faces_z[2, k] = jnp.where(lane < lanes - 1, 0.0, up)
        faces_z[3, k] = jnp.where(lane > 0, 0.0, down)
        diagonals.append(0.5 * diagonal)
    for x in range(planes):
        di, de, m = diagonals[x], diagonals[planes + x], membrane[x]
        determinant = m * di + m * de + di * de
        inverse[0, x] = (di + de) / determinant
        inverse[1, x] = -di / determinant
        inverse[2, x] = (m + di) / determinant
    drain(0)

    def dots(new, others, first_row):
        for offset, other in enumerate(others):
            product = basis[new, 0] * basis[other, 0]
            for k in range(1, total):
                product = product + basis[new, k] * basis[other, k]
            gram[first_row + offset : first_row + offset + 1, :] = jnp.sum(
                product, axis=0, keepdims=True
            )

    def advance(index, restart, between):
        slot = (index + 1) % 2
        values = [None] * total
        for x in range(planes):
            first, second = basis[index, x], basis[index, planes + x]
            v = inverse[0, x] * first + inverse[1, x] * second
            p = inverse[1, x] * first + inverse[2, x] * second
            values[x], values[planes + x] = v + p, p
            field[slot, 0, x] = v + p
            field[slot, 1, x] = p
        set_packs(slot, values, values)
        start(slot)
        sums = []
        for k, (c, x) in enumerate(order):
            value = values[k]
            part = faces_y[0, k] * pltpu.roll(value, rows - 1, 0)
            part = part + faces_y[1, k] * pltpu.roll(value, 1, 0)
            part = part + faces_z[0, k] * pltpu.roll(value, lanes - 1, 1)
            part = part + faces_z[1, k] * pltpu.roll(value, 1, 1)
            if x < planes - 1:
                part = part + faces_x[0, k] * values[k + 1]
            if x > 0:
                part = part + faces_x[1, k] * values[k - 1]
            sums.append(part)
        between()
        finish(slot)
        for k, (c, x) in enumerate(order):
            part = sums[k]
            if x == planes - 1:
                part = part + faces_x[0, k] * halo_x[slot, 1, c]
            if x == 0:
                part = part + faces_x[1, k] * halo_x[slot, 0, c]
            part = part + faces_y[2, k] * halo_y_row(slot, 1, k)
            part = part + faces_y[3, k] * halo_y_row(slot, 0, k)
            part = part + faces_z[2, k] * halo_up_z(slot, k)
            part = part + faces_z[3, k] * halo_down_z(slot, k)
            sums[k] = part
        for x in range(planes):
            first, second = sums[x], sums[x] + sums[planes + x]
            if restart:
                basis[index + 1, x] = 0.5 * first
                basis[index + 1, planes + x] = 0.5 * second
            else:
                basis[index + 1, x] = first - basis[index - 1, x]
                basis[index + 1, planes + x] = second - basis[index - 1, planes + x]
        drain(slot)

    nx, ny, nz = sizes
    devices = nx * ny * nz
    me = (place[0] * ny + place[1]) * nz + place[2]

    def sum_copy(which, target):
        return pltpu.make_async_remote_copy(
            src_ref=parts.at[which, pl.ds(me, 1)],
            dst_ref=parts.at[which, pl.ds(me, 1)],
            send_sem=sum_send.at[which],
            recv_sem=sum_recv.at[which],
            device_id=target,
            device_id_type=MESH,
        )

    def reduced(which):
        ones = jnp.ones((8, lanes), jnp.float32)
        local = lax.dot_general(
            ones, gram[...], (((1,), (1,)), ((), ())), precision=highest,
            preferred_element_type=jnp.float32,
        )
        parts[which, pl.ds(me, 1), :] = local[0:1]
        if devices <= 64:
            for number in range(1, devices):
                dx, dy, dz = number // (ny * nz), number // nz % ny, number % nz
                target = tuple(
                    (place[d] + step) % sizes[d] if step else place[d]
                    for d, step in enumerate((dx, dy, dz))
                )
                sum_copy(which, target).start()
        else:

            def send(number, carry):
                other = (me + number) % devices
                sum_copy(which, (other // (ny * nz), other // nz % ny, other % nz)).start()
                return carry

            lax.fori_loop(1, devices, send, 0)
        everything = pltpu.make_async_remote_copy(
            src_ref=parts.at[which, pl.ds(0, devices - 1)],
            dst_ref=parts.at[which, pl.ds(0, devices - 1)],
            send_sem=sum_send.at[which],
            recv_sem=sum_recv.at[which],
            device_id=((place[0] + 1) % nx, place[1], place[2]),
            device_id_type=MESH,
        )
        everything.wait_recv()
        everything.wait_send()
        summed = jnp.broadcast_to(
            jnp.sum(parts[which], axis=0, keepdims=True), (rows, lanes)
        )

        def entry(number):
            return jnp.broadcast_to(summed[:, number : number + 1], (rows, lanes))

        return entry

    def triangle(j):
        return j * (j + 1) // 2

    for j in range(FIRST):
        advance(j, j == 0, lambda j=j: dots(j, range(j + 1), triangle(j)))
    dots(FIRST, range(FIRST), triangle(FIRST))
    entry = reduced(0)
    matrix = {}
    for j in range(FIRST):
        for i in range(j, FIRST):
            matrix[i, j] = entry(triangle(i) + j)
    factors = cholesky(matrix, FIRST)
    rhs = [entry(triangle(FIRST) + i) for i in range(FIRST)]
    shares = backward_solve(*factors, forward_solve(*factors, rhs))
    at_one = [jnp.full((rows, lanes), TAU[k], jnp.float32) for k in range(FIRST + 1)]
    for i in range(FIRST):
        at_one[FIRST] = at_one[FIRST] - shares[i] * TAU[i]
    for k in range(total):
        value = basis[FIRST, k]
        for i in range(FIRST):
            value = value - shares[i] * basis[i, k]
        basis[FIRST, k] = value

    for j in range(FIRST, KRYLOV):
        advance(j, j == FIRST, lambda j=j: dots(j, range(j + 1), triangle(j)))
        at_one.append(at_one[FIRST] * TAU[j + 1 - FIRST])
    dots(KRYLOV, range(KRYLOV + 1), triangle(KRYLOV))
    entry = reduced(1)
    matrix = {}
    for i in range(KRYLOV + 1):
        for j in range(i + 1):
            matrix[i, j] = entry(triangle(i) + j)
    factors = cholesky(matrix, KRYLOV + 1)
    half = forward_solve(*factors, at_one)
    length = half[0] * half[0]
    for value in half[1:]:
        length = length + value * value
    weights = backward_solve(*factors, [value / length for value in half])

    z = [None] * (KRYLOV + 2)
    z[KRYLOV] = z[KRYLOV + 1] = jnp.zeros((rows, lanes), jnp.float32)
    for i in range(KRYLOV, 0, -1):
        value = weights[i] + (z[i] if i < KRYLOV else 0.0)
        above = z[i + 1] if i + 1 < KRYLOV and i != FIRST - 1 else None
        if i < FIRST:
            extra_term = shares[i] * z[FIRST - 1]
            above = extra_term if above is None else above + extra_term
        if i in (1, FIRST + 1):
            value = value * (1.0 / SCALE)
            above = None if above is None else 0.5 * above
        else:
            value = value * (2.0 / SCALE)
        z[i - 1] = value if above is None else value - above

    for x in range(planes):
        first = z[0] * basis[0, x]
        second = z[0] * basis[0, planes + x]
        for j in range(1, KRYLOV):
            first = first + z[j] * basis[j, x]
            second = second + z[j] * basis[j, planes + x]
        solution_ref[0, x] = inverse[0, x] * first + inverse[1, x] * second
        solution_ref[1, x] = inverse[1, x] * first + inverse[2, x] * second
    for k, (c, x) in enumerate(order):
        value = weights[0] * basis[0, k]
        for j in range(1, KRYLOV + 1):
            value = value + weights[j] * basis[j, k]
        residual_ref[c, x] = value


def solution(mesh):
    sizes = tuple(mesh.shape[axis] for axis in AXES)
    devices = sizes[0] * sizes[1] * sizes[2]

    def body(source, sigma_intra, sigma_extra, membrane):
        planes, rows, lanes = membrane.shape
        total = 2 * planes
        f32 = jnp.float32
        vmem = pl.BlockSpec(memory_space=pltpu.VMEM)
        return pl.pallas_call(
            functools.partial(kernel, sizes),
            out_shape=(jax.ShapeDtypeStruct(source.shape, f32),) * 2,
            in_specs=[vmem] * 4,
            out_specs=(vmem, vmem),
            scratch_shapes=[
                pltpu.VMEM((KRYLOV + 1, total, rows, lanes), f32),
                pltpu.VMEM((2, total, rows, lanes), f32),
                pltpu.VMEM((4, total, rows, lanes), f32),
                pltpu.VMEM((4, total, rows, lanes), f32),
                pltpu.VMEM((3, planes, rows, lanes), f32),
                pltpu.VMEM((2, 2, planes, rows, lanes), f32),
                pltpu.VMEM((2, 2, total, lanes), f32),
                pltpu.VMEM((2, rows, lanes), f32),
                pltpu.VMEM((2, 2, 2, rows, lanes), f32),
                pltpu.VMEM((2, 2, total, lanes), f32),
                pltpu.VMEM((2, 2, rows, lanes), f32),
                pltpu.VMEM((128, lanes), f32),
                pltpu.VMEM((2, devices, 128), f32),
                pltpu.SemaphoreType.DMA((2, 3, 2)),
                pltpu.SemaphoreType.DMA((2, 3, 2)),
                pltpu.SemaphoreType.DMA((2,)),
                pltpu.SemaphoreType.DMA((2,)),
            ],
            compiler_params=pltpu.CompilerParams(has_side_effects=True),
        )(source, sigma_intra, sigma_extra, membrane)

    spec = P(None, "gx", "gy", "gz")
    return jax.shard_map(
        body,
        mesh=mesh,
        in_specs=(spec, spec, spec, P("gx", "gy", "gz")),
        out_specs=(spec, spec),
        check_vma=False,
    )
```

```python
import functools

import jax
import jax.numpy as jnp
from jax import lax
from jax.experimental import pallas as pl
from jax.experimental.pallas import tpu as pltpu
from jax.sharding import PartitionSpec as P

KRYLOV = 10
FIRST = 5
LAG = 3
ORTHO = FIRST + LAG + 1
AXES = ("gx", "gy", "gz")
MESH = pl.DeviceIdType.MESH
highest = lax.Precision.HIGHEST


def cholesky(matrix, count):
    lower = {}
    inverse_diag = []
    for j in range(count):
        pivot = matrix[j, j]
        for m in range(j):
            pivot = pivot - lower[j, m] * lower[j, m]
        inverse_root = lax.rsqrt(pivot)
        inverse_root = inverse_root * (1.5 - 0.5 * pivot * inverse_root * inverse_root)
        inverse_diag.append(inverse_root)
        for i in range(j + 1, count):
            value = matrix[i, j]
            for m in range(j):
                value = value - lower[i, m] * lower[j, m]
            lower[i, j] = value * inverse_root
    return lower, inverse_diag


def forward_solve(lower, inverse_diag, rhs):
    out = []
    for i in range(len(rhs)):
        value = rhs[i]
        for m in range(i):
            value = value - lower[i, m] * out[m]
        out.append(value * inverse_diag[i])
    return out


def backward_solve(lower, inverse_diag, rhs):
    count = len(rhs)
    out = [None] * count
    for i in range(count - 1, -1, -1):
        value = rhs[i]
        for m in range(i + 1, count):
            value = value - lower[m, i] * out[m]
        out[i] = value * inverse_diag[i]
    return out


def kernel(
    sizes,
    source,
    intra,
    extra,
    membrane,
    solution_ref,
    residual_ref,
    basis,
    faces_x,
    faces_y,
    faces_z,
    inverse,
    field,
    pack_y,
    pack_z,
    halo_x,
    halo_y,
    halo_z,
    gram,
    parts,
    send_sem,
    recv_sem,
    sum_send,
    sum_recv,
):
    planes, rows, lanes = source.shape[1:]
    total = 2 * planes
    place = [lax.axis_index(axis) for axis in AXES]
    nx, ny, nz = sizes
    devices = nx * ny * nz
    me = (place[0] * ny + place[1]) * nz + place[2]
    lane = lax.broadcasted_iota(jnp.int32, (rows, lanes), 1)
    row = lax.broadcasted_iota(jnp.int32, (rows, lanes), 0)

    def edge_conditions(dim):
        return (place[dim] > 0, place[dim] < sizes[dim] - 1)

    halos = (halo_x, halo_y, halo_z)

    def send_source(dim, slot, side):
        if dim == 0:
            return field.at[slot, :, planes - 1 if side == 1 else 0]
        if dim == 1:
            return pack_y.at[slot, side]
        return pack_z.at[slot]

    def copy_to(dim, slot, side):
        return pltpu.make_async_remote_copy(
            src_ref=send_source(dim, slot, side),
            dst_ref=halos[dim].at[slot, 1 - side],
            send_sem=send_sem.at[slot, dim, side],
            recv_sem=recv_sem.at[slot, dim, 1 - side],
            device_id={AXES[dim]: place[dim] + (1 if side == 1 else -1)},
            device_id_type=MESH,
        )

    def copy_from(dim, slot, side):
        return pltpu.make_async_remote_copy(
            src_ref=send_source(dim, slot, side),
            dst_ref=halos[dim].at[slot, side],
            send_sem=send_sem.at[slot, dim, side],
            recv_sem=recv_sem.at[slot, dim, side],
            device_id={AXES[dim]: place[dim] + (1 if side == 1 else -1)},
            device_id_type=MESH,
        )

    def each_neighbour(action):
        for dim in (2, 1, 0):
            for side in range(2):
                pl.when(edge_conditions(dim)[side])(functools.partial(action, dim, side))

    def start(slot):
        each_neighbour(lambda dim, side: copy_to(dim, slot, side).start())

    def finish(slot):
        each_neighbour(lambda dim, side: copy_from(dim, slot, side).wait_recv())

    def drain(slot):
        each_neighbour(lambda dim, side: copy_to(dim, slot, side).wait_send())

    def set_packs(slot, values_y, values_z):
        pack_y[slot, 0] = jnp.concatenate([v[0:1] for v in values_y], axis=0)
        pack_y[slot, 1] = jnp.concatenate([v[rows - 1 : rows] for v in values_y], axis=0)
        edges = jnp.zeros((rows, lanes), jnp.float32)
        for k, value in enumerate(values_z):
            turned = pltpu.roll(value, 2 * k + 1, 1)
            edges = jnp.where((lane == 2 * k) | (lane == 2 * k + 1), turned, edges)
        pack_z[slot] = edges

    def zero_edges(dim, side):
        halos[dim][:, side] = jnp.zeros(halos[dim].shape[:1] + halos[dim].shape[2:], jnp.float32)

    for dim in range(3):
        for side in range(2):
            outside = place[dim] == (0 if side == 0 else sizes[dim] - 1)
            pl.when(outside)(functools.partial(zero_edges, dim, side))

    def halo_up_z(slot, k):
        return pltpu.roll(halo_z[slot, 1], lanes - 2 - 2 * k, 1)

    def halo_down_z(slot, k):
        return pltpu.roll(halo_z[slot, 0], (lanes - 2 * k) % lanes, 1)

    def halo_y_row(slot, side, k):
        return jnp.broadcast_to(halo_y[slot, side, k : k + 1, :], (rows, lanes))

    barrier = pltpu.get_barrier_semaphore()
    if sum(sizes) - 3 <= FIRST + 2:
        def greet(dim, side):
            pl.semaphore_signal(
                barrier,
                inc=1,
                device_id={AXES[dim]: place[dim] + (1 if side == 1 else -1)},
                device_id_type=MESH,
            )

        each_neighbour(greet)
        expected = 0
        for dim in range(3):
            for side in range(2):
                expected = expected + edge_conditions(dim)[side].astype(jnp.int32)
        pl.semaphore_wait(barrier, expected)
    else:

        def greet_all(number, carry):
            other = (me + number) % devices
            pl.semaphore_signal(
                barrier,
                inc=1,
                device_id=(other // (ny * nz), other // nz % ny, other % nz),
                device_id_type=MESH,
            )
            return carry

        lax.fori_loop(1, devices, greet_all, 0)
        pl.semaphore_wait(barrier, devices - 1)

    sigma = (intra, extra)
    for c in range(2):
        for x in (0, planes - 1):
            field[0, c, x] = sigma[c][0, x]
    order = [(c, x) for c in range(2) for x in range(planes)]
    set_packs(0, [sigma[c][1, x] for c, x in order], [sigma[c][2, x] for c, x in order])
    start(0)
    gram[...] = jnp.zeros_like(gram)
    for k, (c, x) in enumerate(order):
        basis[0, k] = source[c, x]
    finish(0)
    diagonals = []
    for k, (c, x) in enumerate(order):
        mine = sigma[c][0, x]
        above = sigma[c][0, x + 1] if x < planes - 1 else halo_x[0, 1, c]
        below = sigma[c][0, x - 1] if x > 0 else halo_x[0, 0, c]
        up, down = mine + above, mine + below
        diagonal = up + down
        faces_x[0, k] = up
        faces_x[1, k] = down
        mine = sigma[c][1, x]
        above = jnp.where(row < rows - 1, pltpu.roll(mine, rows - 1, 0), halo_y_row(0, 1, k))
        below = jnp.where(row > 0, pltpu.roll(mine, 1, 0), halo_y_row(0, 0, k))
        up, down = mine + above, mine + below
        diagonal = diagonal + up + down
        faces_y[0, k] = jnp.where(row < rows - 1, up, 0.0)
        faces_y[1, k] = jnp.where(row > 0, down, 0.0)
        faces_y[2, k] = jnp.where(row < rows - 1, 0.0, up)
        faces_y[3, k] = jnp.where(row > 0, 0.0, down)
        mine = sigma[c][2, x]
        above = jnp.where(lane < lanes - 1, pltpu.roll(mine, lanes - 1, 1), halo_up_z(0, k))
        below = jnp.where(lane > 0, pltpu.roll(mine, 1, 1), halo_down_z(0, k))
        up, down = mine + above, mine + below
        diagonal = diagonal + up + down
        faces_z[0, k] = jnp.where(lane < lanes - 1, up, 0.0)
        faces_z[1, k] = jnp.where(lane > 0, down, 0.0)
        faces_z[2, k] = jnp.where(lane < lanes - 1, 0.0, up)
        faces_z[3, k] = jnp.where(lane > 0, 0.0, down)
        diagonals.append(0.5 * diagonal)
    for x in range(planes):
        di, de, m = diagonals[x], diagonals[planes + x], membrane[x]
        determinant = m * di + m * de + di * de
        inverse[0, x] = (di + de) / determinant
        inverse[1, x] = -di / determinant
        inverse[2, x] = (m + di) / determinant
    drain(0)

    def dots(new, others, first_row):
        for offset, other in enumerate(others):
            product = basis[new, 0] * basis[other, 0]
            for k in range(1, total):
                product = product + basis[new, k] * basis[other, k]
            gram[first_row + offset : first_row + offset + 1, :] = jnp.sum(
                product, axis=0, keepdims=True
            )

    def advance(slot, index, restart, between):
        values = [None] * total
        for x in range(planes):
            first, second = basis[index, x], basis[index, planes + x]
            v = inverse[0, x] * first + inverse[1, x] * second
            p = inverse[1, x] * first + inverse[2, x] * second
            values[x], values[planes + x] = v + p, p
            field[slot, 0, x] = v + p
            field[slot, 1, x] = p
        set_packs(slot, values, values)
        start(slot)
        sums = []
        for k, (c, x) in enumerate(order):
            value = values[k]
            part = faces_y[0, k] * pltpu.roll(value, rows - 1, 0)
            part = part + faces_y[1, k] * pltpu.roll(value, 1, 0)
            part = part + faces_z[0, k] * pltpu.roll(value, lanes - 1, 1)
            part = part + faces_z[1, k] * pltpu.roll(value, 1, 1)
            if x < planes - 1:
                part = part + faces_x[0, k] * values[k + 1]
            if x > 0:
                part = part + faces_x[1, k] * values[k - 1]
            sums.append(part)
        between()
        finish(slot)
        for k, (c, x) in enumerate(order):
            part = sums[k]
            if x == planes - 1:
                part = part + faces_x[0, k] * halo_x[slot, 1, c]
            if x == 0:
                part = part + faces_x[1, k] * halo_x[slot, 0, c]
            part = part + faces_y[2, k] * halo_y_row(slot, 1, k)
            part = part + faces_y[3, k] * halo_y_row(slot, 0, k)
            part = part + faces_z[2, k] * halo_up_z(slot, k)
            part = part + faces_z[3, k] * halo_down_z(slot, k)
            sums[k] = part
        for x in range(planes):
            first, second = sums[x], sums[x] + sums[planes + x]
            if restart:
                basis[index + 1, x] = 0.5 * first
                basis[index + 1, planes + x] = 0.5 * second
            else:
                basis[index + 1, x] = first - basis[index - 1, x]
                basis[index + 1, planes + x] = second - basis[index - 1, planes + x]
        drain(slot)

    def sum_copy(which, target):
        return pltpu.make_async_remote_copy(
            src_ref=parts.at[which, pl.ds(me, 1)],
            dst_ref=parts.at[which, pl.ds(me, 1)],
            send_sem=sum_send.at[which],
            recv_sem=sum_recv.at[which],
            device_id=target,
            device_id_type=MESH,
        )

    def start_sum(which):
        ones = jnp.ones((8, lanes), jnp.float32)
        local = lax.dot_general(
            ones, gram[...], (((1,), (1,)), ((), ())), precision=highest,
            preferred_element_type=jnp.float32,
        )
        parts[which, pl.ds(me, 1), :] = local[0:1]
        if devices <= 64:
            for number in range(1, devices):
                dx, dy, dz = number // (ny * nz), number // nz % ny, number % nz
                target = tuple(
                    (place[d] + step) % sizes[d] if step else place[d]
                    for d, step in enumerate((dx, dy, dz))
                )
                sum_copy(which, target).start()
        else:

            def send(number, carry):
                other = (me + number) % devices
                sum_copy(which, (other // (ny * nz), other // nz % ny, other % nz)).start()
                return carry

            lax.fori_loop(1, devices, send, 0)
    def finish_sum(which):
        everything = pltpu.make_async_remote_copy(
            src_ref=parts.at[which, pl.ds(0, devices - 1)],
            dst_ref=parts.at[which, pl.ds(0, devices - 1)],
            send_sem=sum_send.at[which],
            recv_sem=sum_recv.at[which],
            device_id=((place[0] + 1) % nx, place[1], place[2]),
            device_id_type=MESH,
        )
        everything.wait_recv()
        everything.wait_send()
        summed = jnp.broadcast_to(
            jnp.sum(parts[which], axis=0, keepdims=True), (rows, lanes)
        )

        def entry(number):
            return jnp.broadcast_to(summed[:, number : number + 1], (rows, lanes))

        return entry

    def triangle(j):
        return j * (j + 1) // 2

    for j in range(FIRST):
        advance((j + 1) % 2, j, j == 0, lambda j=j: dots(j, range(j + 1), triangle(j)))
    dots(FIRST, range(FIRST), triangle(FIRST))
    start_sum(0)
    found = {}

    def orthonormalise():
        entry = finish_sum(0)
        matrix = {}
        for j in range(FIRST):
            for i in range(j, FIRST):
                matrix[i, j] = entry(triangle(i) + j)
        factors = cholesky(matrix, FIRST)
        on_ortho = forward_solve(*factors, [entry(triangle(FIRST) + i) for i in range(FIRST)])
        shares = backward_solve(*factors, on_ortho)
        at_one = forward_solve(*factors, [jnp.ones((rows, lanes), jnp.float32)] * FIRST)
        last = 1.0 - on_ortho[0] * at_one[0]
        for i in range(1, FIRST):
            last = last - on_ortho[i] * at_one[i]
        found.update(
            factors=factors, shares=shares, at_one=at_one + [last] * (KRYLOV + 1 - FIRST)
        )
        lower, inverse_diag = factors
        for k in range(total):
            made = []
            for i in range(FIRST):
                value = basis[i, k]
                for m in range(i):
                    value = value - lower[i, m] * made[m]
                value = value * inverse_diag[i]
                made.append(value)
                basis[ORTHO + i, k] = value
        for i in range(FIRST):
            dots(ORTHO + i, range(ORTHO, ORTHO + i + 1), triangle(i))

    for j in range(FIRST, FIRST + LAG):
        advance(
            (j + 1) % 2, j, False, orthonormalise if j == FIRST + LAG - 1 else lambda: None
        )
    shares = found["shares"]

    middle = ORTHO + FIRST
    for k in range(total):
        value = basis[FIRST, k]
        for i in range(FIRST):
            value = value - shares[i] * basis[i, k]
        basis[middle, k] = value
        for m in range(1, LAG + 1):
            value = basis[FIRST + m, k] + basis[abs(FIRST - m), k]
            for i in range(FIRST):
                value = value - shares[i] * (basis[i + m, k] + basis[abs(i - m), k])
            basis[middle + m, k] = 0.5 * value
    for j in range(FIRST + LAG, KRYLOV):

        def between(j=j):
            for i in range(FIRST if j == FIRST + LAG else j, j + 1):
                dots(ORTHO + i, range(ORTHO, ORTHO + i + 1), triangle(i))

        advance((j + 1) % 2, ORTHO + j, False, between)
    dots(ORTHO + KRYLOV, range(ORTHO, ORTHO + KRYLOV + 1), triangle(KRYLOV))
    start_sum(1)
    entry = finish_sum(1)
    matrix = {}
    for i in range(KRYLOV + 1):
        for j in range(i + 1):
            matrix[i, j] = entry(triangle(i) + j)
    factors = cholesky(matrix, KRYLOV + 1)
    half = forward_solve(*factors, found["at_one"])
    length = half[0] * half[0]
    for value in half[1:]:
        length = length + value * value
    weights = backward_solve(*factors, [value / length for value in half])

    target = backward_solve(*found["factors"], weights[:FIRST]) + weights[FIRST:]
    z = [None] * KRYLOV
    for i in range(KRYLOV, 0, -1):
        value = target[i] + z[i] if i < KRYLOV else target[i]
        above = z[i + 1] if i + 1 < KRYLOV and i != FIRST - 1 else None
        if i < FIRST:
            share = shares[i] * z[FIRST - 1]
            above = share if above is None else above + share
        if i in (1, FIRST + 1):
            z[i - 1] = value - 0.5 * above
        else:
            z[i - 1] = 2.0 * value if above is None else 2.0 * value - above

    for x in range(planes):
        first = z[0] * basis[0, x]
        second = z[0] * basis[0, planes + x]
        for j in range(1, KRYLOV):
            at = j if j < FIRST else ORTHO + j
            first = first + z[j] * basis[at, x]
            second = second + z[j] * basis[at, planes + x]
        solution_ref[0, x] = inverse[0, x] * first + inverse[1, x] * second
        solution_ref[1, x] = inverse[1, x] * first + inverse[2, x] * second
    for k, (c, x) in enumerate(order):
        value = weights[0] * basis[ORTHO, k]
        for j in range(1, KRYLOV + 1):
            value = value + weights[j] * basis[ORTHO + j, k]
        residual_ref[c, x] = value


def solution(mesh):
    sizes = tuple(mesh.shape[axis] for axis in AXES)
    devices = sizes[0] * sizes[1] * sizes[2]

    def body(source, sigma_intra, sigma_extra, membrane):
        planes, rows, lanes = membrane.shape
        total = 2 * planes
        f32 = jnp.float32
        vmem = pl.BlockSpec(memory_space=pltpu.VMEM)
        return pl.pallas_call(
            functools.partial(kernel, sizes),
            out_shape=(jax.ShapeDtypeStruct(source.shape, f32),) * 2,
            in_specs=[vmem] * 4,
            out_specs=(vmem, vmem),
            scratch_shapes=[
                pltpu.VMEM((ORTHO + KRYLOV + 1, total, rows, lanes), f32),
                pltpu.VMEM((2, total, rows, lanes), f32),
                pltpu.VMEM((4, total, rows, lanes), f32),
                pltpu.VMEM((4, total, rows, lanes), f32),
                pltpu.VMEM((3, planes, rows, lanes), f32),
                pltpu.VMEM((2, 2, planes, rows, lanes), f32),
                pltpu.VMEM((2, 2, total, lanes), f32),
                pltpu.VMEM((2, rows, lanes), f32),
                pltpu.VMEM((2, 2, 2, rows, lanes), f32),
                pltpu.VMEM((2, 2, total, lanes), f32),
                pltpu.VMEM((2, 2, rows, lanes), f32),
                pltpu.VMEM((128, lanes), f32),
                pltpu.VMEM((2, devices, 128), f32),
                pltpu.SemaphoreType.DMA((2, 3, 2)),
                pltpu.SemaphoreType.DMA((2, 3, 2)),
                pltpu.SemaphoreType.DMA((2,)),
                pltpu.SemaphoreType.DMA((2,)),
            ],
            compiler_params=pltpu.CompilerParams(collective_id=0, has_side_effects=True),
        )(source, sigma_intra, sigma_extra, membrane)

    spec = P(None, "gx", "gy", "gz")
    return jax.shard_map(
        body,
        mesh=mesh,
        in_specs=(spec, spec, spec, P("gx", "gy", "gz")),
        out_specs=(spec, spec),
        check_vma=False,
    )
```

```python
import functools

import jax
import jax.numpy as jnp
from jax import lax
from jax.experimental import pallas as pl
from jax.experimental.pallas import tpu as pltpu
from jax.sharding import PartitionSpec as P

KRYLOV = 10
FIRST = 5
LAG = 3
ORTHO = FIRST + LAG + 1
AXES = ("gx", "gy", "gz")
MESH = pl.DeviceIdType.MESH
highest = lax.Precision.HIGHEST


def cholesky(matrix, count):
    lower = {}
    inverse_diag = []
    for j in range(count):
        pivot = matrix[j, j]
        for m in range(j):
            pivot = pivot - lower[j, m] * lower[j, m]
        inverse_root = lax.rsqrt(pivot)
        inverse_root = inverse_root * (1.5 - 0.5 * pivot * inverse_root * inverse_root)
        inverse_diag.append(inverse_root)
        for i in range(j + 1, count):
            value = matrix[i, j]
            for m in range(j):
                value = value - lower[i, m] * lower[j, m]
            lower[i, j] = value * inverse_root
    return lower, inverse_diag


def forward_solve(lower, inverse_diag, rhs):
    out = []
    for i in range(len(rhs)):
        value = rhs[i]
        for m in range(i):
            value = value - lower[i, m] * out[m]
        out.append(value * inverse_diag[i])
    return out


def backward_solve(lower, inverse_diag, rhs):
    count = len(rhs)
    out = [None] * count
    for i in range(count - 1, -1, -1):
        value = rhs[i]
        for m in range(i + 1, count):
            value = value - lower[m, i] * out[m]
        out[i] = value * inverse_diag[i]
    return out


def kernel(
    sizes,
    source_hbm,
    intra_hbm,
    extra_hbm,
    membrane_hbm,
    solution_ref,
    residual_ref,
    basis,
    faces_x,
    faces_y,
    faces_z,
    inverse,
    field,
    pack_y,
    pack_z,
    halo_x,
    halo_y,
    halo_z,
    gram,
    parts,
    send_sem,
    recv_sem,
    sum_send,
    sum_recv,
    intra,
    extra,
    membrane,
    input_sem,
):
    planes, rows, lanes = membrane_hbm.shape
    total = 2 * planes
    place = [lax.axis_index(axis) for axis in AXES]
    nx, ny, nz = sizes
    devices = nx * ny * nz
    me = (place[0] * ny + place[1]) * nz + place[2]
    lane = lax.broadcasted_iota(jnp.int32, (rows, lanes), 1)
    row = lax.broadcasted_iota(jnp.int32, (rows, lanes), 0)

    def edge_conditions(dim):
        return (place[dim] > 0, place[dim] < sizes[dim] - 1)

    halos = (halo_x, halo_y, halo_z)

    def send_source(dim, slot, side):
        if dim == 0:
            return field.at[slot, :, planes - 1 if side == 1 else 0]
        if dim == 1:
            return pack_y.at[slot, side]
        return pack_z.at[slot]

    def copy_to(dim, slot, side):
        return pltpu.make_async_remote_copy(
            src_ref=send_source(dim, slot, side),
            dst_ref=halos[dim].at[slot, 1 - side],
            send_sem=send_sem.at[slot, dim, side],
            recv_sem=recv_sem.at[slot, dim, 1 - side],
            device_id={AXES[dim]: place[dim] + (1 if side == 1 else -1)},
            device_id_type=MESH,
        )

    def copy_from(dim, slot, side):
        return pltpu.make_async_remote_copy(
            src_ref=send_source(dim, slot, side),
            dst_ref=halos[dim].at[slot, side],
            send_sem=send_sem.at[slot, dim, side],
            recv_sem=recv_sem.at[slot, dim, side],
            device_id={AXES[dim]: place[dim] + (1 if side == 1 else -1)},
            device_id_type=MESH,
        )

    def each_neighbour(action, dims=(2, 1, 0)):
        for dim in dims:
            for side in range(2):
                pl.when(edge_conditions(dim)[side])(functools.partial(action, dim, side))

    def start(slot, dims):
        each_neighbour(lambda dim, side: copy_to(dim, slot, side).start(), dims)

    def finish(slot):
        each_neighbour(lambda dim, side: copy_from(dim, slot, side).wait_recv())

    def drain(slot):
        each_neighbour(lambda dim, side: copy_to(dim, slot, side).wait_send())

    def set_pack_y(slot, values_y):
        pack_y[slot, 0] = jnp.concatenate([v[0:1] for v in values_y], axis=0)
        pack_y[slot, 1] = jnp.concatenate([v[rows - 1 : rows] for v in values_y], axis=0)

    def set_pack_z(slot, values_z):
        edges = jnp.zeros((rows, lanes), jnp.float32)
        for k, value in enumerate(values_z):
            turned = pltpu.roll(value, 2 * k + 1, 1)
            edges = jnp.where((lane == 2 * k) | (lane == 2 * k + 1), turned, edges)
        pack_z[slot] = edges

    def zero_edges(dim, side):
        halos[dim][:, side] = jnp.zeros(halos[dim].shape[:1] + halos[dim].shape[2:], jnp.float32)

    for dim in range(3):
        for side in range(2):
            outside = place[dim] == (0 if side == 0 else sizes[dim] - 1)
            pl.when(outside)(functools.partial(zero_edges, dim, side))

    def halo_up_z(slot, k):
        return pltpu.roll(halo_z[slot, 1], lanes - 2 - 2 * k, 1)

    def halo_down_z(slot, k):
        return pltpu.roll(halo_z[slot, 0], (lanes - 2 * k) % lanes, 1)

    def halo_y_row(slot, side, k):
        return jnp.broadcast_to(halo_y[slot, side, k : k + 1, :], (rows, lanes))

    loads = [
        pltpu.make_async_copy(intra_hbm, intra, input_sem.at[0]),
        pltpu.make_async_copy(extra_hbm, extra, input_sem.at[1]),
        pltpu.make_async_copy(membrane_hbm, membrane, input_sem.at[2]),
        pltpu.make_async_copy(source_hbm, basis.at[0], input_sem.at[3]),
    ]
    for load in loads:
        load.start()
    barrier = pltpu.get_barrier_semaphore()
    if sum(sizes) - 3 <= FIRST + 2:
        def greet(dim, side):
            pl.semaphore_signal(
                barrier,
                inc=1,
                device_id={AXES[dim]: place[dim] + (1 if side == 1 else -1)},
                device_id_type=MESH,
            )

        each_neighbour(greet)
        expected = 0
        for dim in range(3):
            for side in range(2):
                expected = expected + edge_conditions(dim)[side].astype(jnp.int32)
    else:

        def greet_all(number, carry):
            other = (me + number) % devices
            pl.semaphore_signal(
                barrier,
                inc=1,
                device_id=(other // (ny * nz), other // nz % ny, other % nz),
                device_id_type=MESH,
            )
            return carry

        lax.fori_loop(1, devices, greet_all, 0)
        expected = devices - 1

    sigma = (intra, extra)
    loads[0].wait()
    loads[1].wait()
    for c in range(2):
        for x in (0, planes - 1):
            field[0, c, x] = sigma[c][0, x]
    order = [(c, x) for c in range(2) for x in range(planes)]
    set_pack_y(0, [sigma[c][1, x] for c, x in order])
    set_pack_z(0, [sigma[c][2, x] for c, x in order])
    pl.semaphore_wait(barrier, expected)
    start(0, (0, 1, 2))
    gram[...] = jnp.zeros_like(gram)
    loads[2].wait()
    loads[3].wait()
    finish(0)
    diagonals = []
    for k, (c, x) in enumerate(order):
        mine = sigma[c][0, x]
        above = sigma[c][0, x + 1] if x < planes - 1 else halo_x[0, 1, c]
        below = sigma[c][0, x - 1] if x > 0 else halo_x[0, 0, c]
        up, down = mine + above, mine + below
        diagonal = up + down
        faces_x[0, k] = up
        faces_x[1, k] = down
        mine = sigma[c][1, x]
        above = jnp.where(row < rows - 1, pltpu.roll(mine, rows - 1, 0), halo_y_row(0, 1, k))
        below = jnp.where(row > 0, pltpu.roll(mine, 1, 0), halo_y_row(0, 0, k))
        up, down = mine + above, mine + below
        diagonal = diagonal + up + down
        faces_y[0, k] = jnp.where(row < rows - 1, up, 0.0)
        faces_y[1, k] = jnp.where(row > 0, down, 0.0)
        faces_y[2, k] = jnp.where(row < rows - 1, 0.0, up)
        faces_y[3, k] = jnp.where(row > 0, 0.0, down)
        mine = sigma[c][2, x]
        above = jnp.where(lane < lanes - 1, pltpu.roll(mine, lanes - 1, 1), halo_up_z(0, k))
        below = jnp.where(lane > 0, pltpu.roll(mine, 1, 1), halo_down_z(0, k))
        up, down = mine + above, mine + below
        diagonal = diagonal + up + down
        faces_z[0, k] = jnp.where(lane < lanes - 1, up, 0.0)
        faces_z[1, k] = jnp.where(lane > 0, down, 0.0)
        faces_z[2, k] = jnp.where(lane < lanes - 1, 0.0, up)
        faces_z[3, k] = jnp.where(lane > 0, 0.0, down)
        diagonals.append(0.5 * diagonal)
    for x in range(planes):
        di, de, m = diagonals[x], diagonals[planes + x], membrane[x]
        determinant = m * di + m * de + di * de
        inverse[0, x] = (di + de) / determinant
        inverse[1, x] = -di / determinant
        inverse[2, x] = (m + di) / determinant

    def dots(new, others, first_row):
        for offset, other in enumerate(others):
            product = basis[new, 0] * basis[other, 0]
            for k in range(1, total):
                product = product + basis[new, k] * basis[other, k]
            gram[first_row + offset : first_row + offset + 1, :] = jnp.sum(
                product, axis=0, keepdims=True
            )

    def advance(slot, index, restart, between):
        values = [None] * total
        for x in range(planes):
            first, second = basis[index, x], basis[index, planes + x]
            v = inverse[0, x] * first + inverse[1, x] * second
            p = inverse[1, x] * first + inverse[2, x] * second
            values[x], values[planes + x] = v + p, p
            field[slot, 0, x] = v + p
            field[slot, 1, x] = p
        start(slot, (0,))
        set_pack_y(slot, values)
        start(slot, (1,))
        set_pack_z(slot, values)
        start(slot, (2,))
        sums = []
        for k, (c, x) in enumerate(order):
            value = values[k]
            part = faces_y[0, k] * pltpu.roll(value, rows - 1, 0)
            part = part + faces_y[1, k] * pltpu.roll(value, 1, 0)
            part = part + faces_z[0, k] * pltpu.roll(value, lanes - 1, 1)
            part = part + faces_z[1, k] * pltpu.roll(value, 1, 1)
            if x < planes - 1:
                part = part + faces_x[0, k] * values[k + 1]
            if x > 0:
                part = part + faces_x[1, k] * values[k - 1]
            sums.append(part)
        between()
        drain(1 - slot)
        finish(slot)
        for k, (c, x) in enumerate(order):
            part = sums[k]
            if x == planes - 1:
                part = part + faces_x[0, k] * halo_x[slot, 1, c]
            if x == 0:
                part = part + faces_x[1, k] * halo_x[slot, 0, c]
            part = part + faces_y[2, k] * halo_y_row(slot, 1, k)
            part = part + faces_y[3, k] * halo_y_row(slot, 0, k)
            part = part + faces_z[2, k] * halo_up_z(slot, k)
            part = part + faces_z[3, k] * halo_down_z(slot, k)
            sums[k] = part
        for x in range(planes):
            first, second = sums[x], sums[x] + sums[planes + x]
            if restart:
                basis[index + 1, x] = 0.5 * first
                basis[index + 1, planes + x] = 0.5 * second
            else:
                basis[index + 1, x] = first - basis[index - 1, x]
                basis[index + 1, planes + x] = second - basis[index - 1, planes + x]

    def sum_copy(which, target):
        return pltpu.make_async_remote_copy(
            src_ref=parts.at[which, pl.ds(me, 1)],
            dst_ref=parts.at[which, pl.ds(me, 1)],
            send_sem=sum_send.at[which],
            recv_sem=sum_recv.at[which],
            device_id=target,
            device_id_type=MESH,
        )

    def start_sum(which):
        ones = jnp.ones((8, lanes), jnp.float32)
        local = lax.dot_general(
            ones, gram[...], (((1,), (1,)), ((), ())), precision=highest,
            preferred_element_type=jnp.float32,
        )
        parts[which, pl.ds(me, 1), :] = local[0:1]
        if devices <= 64:
            for number in range(1, devices):
                dx, dy, dz = number // (ny * nz), number // nz % ny, number % nz
                target = tuple(
                    (place[d] + step) % sizes[d] if step else place[d]
                    for d, step in enumerate((dx, dy, dz))
                )
                sum_copy(which, target).start()
        else:

            def send(number, carry):
                other = (me + number) % devices
                sum_copy(which, (other // (ny * nz), other // nz % ny, other % nz)).start()
                return carry

            lax.fori_loop(1, devices, send, 0)
    def finish_sum(which):
        everything = pltpu.make_async_remote_copy(
            src_ref=parts.at[which, pl.ds(0, devices - 1)],
            dst_ref=parts.at[which, pl.ds(0, devices - 1)],
            send_sem=sum_send.at[which],
            recv_sem=sum_recv.at[which],
            device_id=((place[0] + 1) % nx, place[1], place[2]),
            device_id_type=MESH,
        )
        everything.wait_recv()
        everything.wait_send()
        summed = jnp.broadcast_to(
            jnp.sum(parts[which], axis=0, keepdims=True), (rows, lanes)
        )

        def entry(number):
            return jnp.broadcast_to(summed[:, number : number + 1], (rows, lanes))

        return entry

    def triangle(j):
        return j * (j + 1) // 2

    for j in range(FIRST):
        advance((j + 1) % 2, j, j == 0, lambda j=j: dots(j, range(j + 1), triangle(j)))
    dots(FIRST, range(FIRST), triangle(FIRST))
    start_sum(0)
    found = {}

    def orthonormalise():
        entry = finish_sum(0)
        matrix = {}
        for j in range(FIRST):
            for i in range(j, FIRST):
                matrix[i, j] = entry(triangle(i) + j)
        factors = cholesky(matrix, FIRST)
        on_ortho = forward_solve(*factors, [entry(triangle(FIRST) + i) for i in range(FIRST)])
        shares = backward_solve(*factors, on_ortho)
        at_one = forward_solve(*factors, [jnp.ones((rows, lanes), jnp.float32)] * FIRST)
        last = 1.0 - on_ortho[0] * at_one[0]
        for i in range(1, FIRST):
            last = last - on_ortho[i] * at_one[i]
        found.update(
            factors=factors, shares=shares, at_one=at_one + [last] * (KRYLOV + 1 - FIRST)
        )
        lower, inverse_diag = factors
        for k in range(total):
            made = []
            for i in range(FIRST):
                value = basis[i, k]
                for m in range(i):
                    value = value - lower[i, m] * made[m]
                value = value * inverse_diag[i]
                made.append(value)
                basis[ORTHO + i, k] = value
        for i in range(FIRST):
            dots(ORTHO + i, range(ORTHO, ORTHO + i + 1), triangle(i))

    for j in range(FIRST, FIRST + LAG):
        advance(
            (j + 1) % 2, j, False, orthonormalise if j == FIRST + LAG - 1 else lambda: None
        )
    shares = found["shares"]

    middle = ORTHO + FIRST
    for k in range(total):
        value = basis[FIRST, k]
        for i in range(FIRST):
            value = value - shares[i] * basis[i, k]
        basis[middle, k] = value
        for m in range(1, LAG + 1):
            value = basis[FIRST + m, k] + basis[abs(FIRST - m), k]
            for i in range(FIRST):
                value = value - shares[i] * (basis[i + m, k] + basis[abs(i - m), k])
            basis[middle + m, k] = 0.5 * value
    for j in range(FIRST + LAG, KRYLOV):

        def between(j=j):
            for i in range(FIRST if j == FIRST + LAG else j, j + 1):
                dots(ORTHO + i, range(ORTHO, ORTHO + i + 1), triangle(i))

        advance((j + 1) % 2, ORTHO + j, False, between)
    dots(ORTHO + KRYLOV, range(ORTHO, ORTHO + KRYLOV + 1), triangle(KRYLOV))
    start_sum(1)
    drain(KRYLOV % 2)
    entry = finish_sum(1)
    matrix = {}
    for i in range(KRYLOV + 1):
        for j in range(i + 1):
            matrix[i, j] = entry(triangle(i) + j)
    factors = cholesky(matrix, KRYLOV + 1)
    half = forward_solve(*factors, found["at_one"])
    length = half[0] * half[0]
    for value in half[1:]:
        length = length + value * value
    weights = backward_solve(*factors, [value / length for value in half])

    target = backward_solve(*found["factors"], weights[:FIRST]) + weights[FIRST:]
    z = [None] * KRYLOV
    for i in range(KRYLOV, 0, -1):
        value = target[i] + z[i] if i < KRYLOV else target[i]
        above = z[i + 1] if i + 1 < KRYLOV and i != FIRST - 1 else None
        if i < FIRST:
            share = shares[i] * z[FIRST - 1]
            above = share if above is None else above + share
        if i in (1, FIRST + 1):
            z[i - 1] = value - 0.5 * above
        else:
            z[i - 1] = 2.0 * value if above is None else 2.0 * value - above

    for x in range(planes):
        first = z[0] * basis[0, x]
        second = z[0] * basis[0, planes + x]
        for j in range(1, KRYLOV):
            at = j if j < FIRST else ORTHO + j
            first = first + z[j] * basis[at, x]
            second = second + z[j] * basis[at, planes + x]
        solution_ref[0, x] = inverse[0, x] * first + inverse[1, x] * second
        solution_ref[1, x] = inverse[1, x] * first + inverse[2, x] * second
    for k, (c, x) in enumerate(order):
        value = weights[0] * basis[ORTHO, k]
        for j in range(1, KRYLOV + 1):
            value = value + weights[j] * basis[ORTHO + j, k]
        residual_ref[c, x] = value


def solution(mesh):
    sizes = tuple(mesh.shape[axis] for axis in AXES)
    devices = sizes[0] * sizes[1] * sizes[2]

    def body(source, sigma_intra, sigma_extra, membrane):
        planes, rows, lanes = membrane.shape
        total = 2 * planes
        f32 = jnp.float32
        vmem = pl.BlockSpec(memory_space=pltpu.VMEM)
        return pl.pallas_call(
            functools.partial(kernel, sizes),
            out_shape=(jax.ShapeDtypeStruct(source.shape, f32),) * 2,
            in_specs=[pl.BlockSpec(memory_space=pl.ANY)] * 4,
            out_specs=(vmem, vmem),
            scratch_shapes=[
                pltpu.VMEM((ORTHO + KRYLOV + 1, total, rows, lanes), f32),
                pltpu.VMEM((2, total, rows, lanes), f32),
                pltpu.VMEM((4, total, rows, lanes), f32),
                pltpu.VMEM((4, total, rows, lanes), f32),
                pltpu.VMEM((3, planes, rows, lanes), f32),
                pltpu.VMEM((2, 2, planes, rows, lanes), f32),
                pltpu.VMEM((2, 2, total, lanes), f32),
                pltpu.VMEM((2, rows, lanes), f32),
                pltpu.VMEM((2, 2, 2, rows, lanes), f32),
                pltpu.VMEM((2, 2, total, lanes), f32),
                pltpu.VMEM((2, 2, rows, lanes), f32),
                pltpu.VMEM((128, lanes), f32),
                pltpu.VMEM((2, devices, 128), f32),
                pltpu.SemaphoreType.DMA((2, 3, 2)),
                pltpu.SemaphoreType.DMA((2, 3, 2)),
                pltpu.SemaphoreType.DMA((2,)),
                pltpu.SemaphoreType.DMA((2,)),
                pltpu.VMEM(sigma_intra.shape, f32),
                pltpu.VMEM(sigma_extra.shape, f32),
                pltpu.VMEM(membrane.shape, f32),
                pltpu.SemaphoreType.DMA((4,)),
            ],
            compiler_params=pltpu.CompilerParams(collective_id=0, has_side_effects=True),
        )(source.reshape(total, rows, lanes), sigma_intra, sigma_extra, membrane)

    spec = P(None, "gx", "gy", "gz")
    return jax.shard_map(
        body,
        mesh=mesh,
        in_specs=(spec, spec, spec, P("gx", "gy", "gz")),
        out_specs=(spec, spec),
        check_vma=False,
    )
```

```python
import functools

import jax
import jax.numpy as jnp
from jax import lax
from jax.experimental import pallas as pl
from jax.experimental.pallas import tpu as pltpu
from jax.sharding import PartitionSpec as P

KRYLOV = 10
FIRST = 5
LAG = 3
ORTHO = FIRST + LAG + 1
AXES = ("gx", "gy", "gz")
MESH = pl.DeviceIdType.MESH
highest = lax.Precision.HIGHEST


def cholesky(matrix, count):
    lower = {}
    inverse_diag = []
    for j in range(count):
        pivot = matrix[j, j]
        for m in range(j):
            pivot = pivot - lower[j, m] * lower[j, m]
        inverse_root = lax.rsqrt(pivot)
        inverse_root = inverse_root * (1.5 - 0.5 * pivot * inverse_root * inverse_root)
        inverse_diag.append(inverse_root)
        for i in range(j + 1, count):
            value = matrix[i, j]
            for m in range(j):
                value = value - lower[i, m] * lower[j, m]
            lower[i, j] = value * inverse_root
    return lower, inverse_diag


def forward_solve(lower, inverse_diag, rhs):
    out = []
    for i in range(len(rhs)):
        value = rhs[i]
        for m in range(i):
            value = value - lower[i, m] * out[m]
        out.append(value * inverse_diag[i])
    return out


def backward_solve(lower, inverse_diag, rhs):
    count = len(rhs)
    out = [None] * count
    for i in range(count - 1, -1, -1):
        value = rhs[i]
        for m in range(i + 1, count):
            value = value - lower[m, i] * out[m]
        out[i] = value * inverse_diag[i]
    return out


def kernel(
    sizes,
    source_hbm,
    intra_hbm,
    extra_hbm,
    membrane_hbm,
    solution_ref,
    residual_ref,
    basis,
    faces_x,
    faces_y,
    faces_z,
    inverse,
    field,
    pack_y,
    pack_z,
    halo_x,
    halo_y,
    halo_z,
    gram,
    parts,
    send_sem,
    recv_sem,
    sum_send,
    sum_recv,
    intra,
    extra,
    membrane,
    input_sem,
):
    planes, rows, lanes = membrane_hbm.shape
    total = 2 * planes
    place = [lax.axis_index(axis) for axis in AXES]
    nx, ny, nz = sizes
    devices = nx * ny * nz
    me = (place[0] * ny + place[1]) * nz + place[2]
    lane = lax.broadcasted_iota(jnp.int32, (rows, lanes), 1)
    row = lax.broadcasted_iota(jnp.int32, (rows, lanes), 0)

    def edge_conditions(dim):
        return (place[dim] > 0, place[dim] < sizes[dim] - 1)

    halos = (halo_x, halo_y, halo_z)

    def send_source(dim, slot, side):
        if dim == 0:
            return field.at[slot, :, planes - 1 if side == 1 else 0]
        if dim == 1:
            return pack_y.at[slot, side]
        return pack_z.at[slot]

    def copy_to(dim, slot, side):
        return pltpu.make_async_remote_copy(
            src_ref=send_source(dim, slot, side),
            dst_ref=halos[dim].at[slot, 1 - side],
            send_sem=send_sem.at[slot, dim, side],
            recv_sem=recv_sem.at[slot, dim, 1 - side],
            device_id={AXES[dim]: place[dim] + (1 if side == 1 else -1)},
            device_id_type=MESH,
        )

    def copy_from(dim, slot, side):
        return pltpu.make_async_remote_copy(
            src_ref=send_source(dim, slot, side),
            dst_ref=halos[dim].at[slot, side],
            send_sem=send_sem.at[slot, dim, side],
            recv_sem=recv_sem.at[slot, dim, side],
            device_id={AXES[dim]: place[dim] + (1 if side == 1 else -1)},
            device_id_type=MESH,
        )

    def each_neighbour(action, dims=(2, 1, 0)):
        for dim in dims:
            for side in range(2):
                pl.when(edge_conditions(dim)[side])(functools.partial(action, dim, side))

    def start(slot, dims):
        each_neighbour(lambda dim, side: copy_to(dim, slot, side).start(), dims)

    def finish(slot, dims=(0, 1, 2)):
        each_neighbour(lambda dim, side: copy_from(dim, slot, side).wait_recv(), dims)

    def drain(slot):
        each_neighbour(lambda dim, side: copy_to(dim, slot, side).wait_send())

    def set_pack_y(slot, values_y):
        pack_y[slot, 0] = jnp.concatenate([v[0:1] for v in values_y], axis=0)
        pack_y[slot, 1] = jnp.concatenate([v[rows - 1 : rows] for v in values_y], axis=0)

    def set_pack_z(slot, values_z):
        edges = jnp.zeros((rows, lanes), jnp.float32)
        for k, value in enumerate(values_z):
            turned = pltpu.roll(value, 2 * k + 1, 1)
            edges = jnp.where((lane == 2 * k) | (lane == 2 * k + 1), turned, edges)
        pack_z[slot] = edges

    def zero_edges(dim, side):
        halos[dim][:, side] = jnp.zeros(halos[dim].shape[:1] + halos[dim].shape[2:], jnp.float32)

    for dim in range(3):
        for side in range(2):
            outside = place[dim] == (0 if side == 0 else sizes[dim] - 1)
            pl.when(outside)(functools.partial(zero_edges, dim, side))

    def halo_up_z(slot, k):
        return pltpu.roll(halo_z[slot, 1], lanes - 2 - 2 * k, 1)

    def halo_down_z(slot, k):
        return pltpu.roll(halo_z[slot, 0], (lanes - 2 * k) % lanes, 1)

    def halo_y_row(slot, side, k):
        return jnp.broadcast_to(halo_y[slot, side, k : k + 1, :], (rows, lanes))

    loads = [
        pltpu.make_async_copy(intra_hbm, intra, input_sem.at[0]),
        pltpu.make_async_copy(extra_hbm, extra, input_sem.at[1]),
        pltpu.make_async_copy(membrane_hbm, membrane, input_sem.at[2]),
        pltpu.make_async_copy(source_hbm, basis.at[0], input_sem.at[3]),
    ]
    for load in loads:
        load.start()
    barrier = pltpu.get_barrier_semaphore()
    if sum(sizes) - 3 <= FIRST + 2:
        def greet(dim, side):
            pl.semaphore_signal(
                barrier,
                inc=1,
                device_id={AXES[dim]: place[dim] + (1 if side == 1 else -1)},
                device_id_type=MESH,
            )

        each_neighbour(greet)
        expected = 0
        for dim in range(3):
            for side in range(2):
                expected = expected + edge_conditions(dim)[side].astype(jnp.int32)
    else:

        def greet_all(number, carry):
            other = (me + number) % devices
            pl.semaphore_signal(
                barrier,
                inc=1,
                device_id=(other // (ny * nz), other // nz % ny, other % nz),
                device_id_type=MESH,
            )
            return carry

        lax.fori_loop(1, devices, greet_all, 0)
        expected = devices - 1

    sigma = (intra, extra)
    loads[0].wait()
    loads[1].wait()
    for c in range(2):
        for x in (0, planes - 1):
            field[0, c, x] = sigma[c][0, x]
    order = [(c, x) for c in range(2) for x in range(planes)]
    set_pack_y(0, [sigma[c][1, x] for c, x in order])
    set_pack_z(0, [sigma[c][2, x] for c, x in order])
    pl.semaphore_wait(barrier, expected)
    start(0, (0, 1, 2))
    gram[...] = jnp.zeros_like(gram)
    loads[2].wait()
    loads[3].wait()
    finish(0)
    diagonals = []
    for k, (c, x) in enumerate(order):
        mine = sigma[c][0, x]
        above = sigma[c][0, x + 1] if x < planes - 1 else halo_x[0, 1, c]
        below = sigma[c][0, x - 1] if x > 0 else halo_x[0, 0, c]
        up, down = mine + above, mine + below
        diagonal = up + down
        faces_x[0, k] = up
        faces_x[1, k] = down
        mine = sigma[c][1, x]
        above = jnp.where(row < rows - 1, pltpu.roll(mine, rows - 1, 0), halo_y_row(0, 1, k))
        below = jnp.where(row > 0, pltpu.roll(mine, 1, 0), halo_y_row(0, 0, k))
        up, down = mine + above, mine + below
        diagonal = diagonal + up + down
        faces_y[0, k] = jnp.where(row < rows - 1, up, 0.0)
        faces_y[1, k] = jnp.where(row > 0, down, 0.0)
        faces_y[2, k] = jnp.where(row < rows - 1, 0.0, up)
        faces_y[3, k] = jnp.where(row > 0, 0.0, down)
        mine = sigma[c][2, x]
        above = jnp.where(lane < lanes - 1, pltpu.roll(mine, lanes - 1, 1), halo_up_z(0, k))
        below = jnp.where(lane > 0, pltpu.roll(mine, 1, 1), halo_down_z(0, k))
        up, down = mine + above, mine + below
        diagonal = diagonal + up + down
        faces_z[0, k] = jnp.where(lane < lanes - 1, up, 0.0)
        faces_z[1, k] = jnp.where(lane > 0, down, 0.0)
        faces_z[2, k] = jnp.where(lane < lanes - 1, 0.0, up)
        faces_z[3, k] = jnp.where(lane > 0, 0.0, down)
        diagonals.append(0.5 * diagonal)
    for x in range(planes):
        di, de, m = diagonals[x], diagonals[planes + x], membrane[x]
        determinant = m * di + m * de + di * de
        inverse[0, x] = (di + de) / determinant
        inverse[1, x] = -di / determinant
        inverse[2, x] = (m + di) / determinant

    def dots(new, others, first_row):
        for offset, other in enumerate(others):
            product = basis[new, 0] * basis[other, 0]
            for k in range(1, total):
                product = product + basis[new, k] * basis[other, k]
            gram[first_row + offset : first_row + offset + 1, :] = jnp.sum(
                product, axis=0, keepdims=True
            )

    def advance(slot, index, restart, between):
        values = [None] * total
        for x in range(planes):
            first, second = basis[index, x], basis[index, planes + x]
            v = inverse[0, x] * first + inverse[1, x] * second
            p = inverse[1, x] * first + inverse[2, x] * second
            values[x], values[planes + x] = v + p, p
            field[slot, 0, x] = v + p
            field[slot, 1, x] = p
        start(slot, (0,))
        set_pack_y(slot, values)
        start(slot, (1,))
        set_pack_z(slot, values)
        start(slot, (2,))
        sums = []
        for k, (c, x) in enumerate(order):
            value = values[k]
            part = faces_y[0, k] * pltpu.roll(value, rows - 1, 0)
            part = part + faces_y[1, k] * pltpu.roll(value, 1, 0)
            part = part + faces_z[0, k] * pltpu.roll(value, lanes - 1, 1)
            part = part + faces_z[1, k] * pltpu.roll(value, 1, 1)
            if x < planes - 1:
                part = part + faces_x[0, k] * values[k + 1]
            if x > 0:
                part = part + faces_x[1, k] * values[k - 1]
            sums.append(part)
        between()
        drain(1 - slot)
        finish(slot, (0, 1))
        for k, (c, x) in enumerate(order):
            part = sums[k]
            if x == planes - 1:
                part = part + faces_x[0, k] * halo_x[slot, 1, c]
            if x == 0:
                part = part + faces_x[1, k] * halo_x[slot, 0, c]
            part = part + faces_y[2, k] * halo_y_row(slot, 1, k)
            part = part + faces_y[3, k] * halo_y_row(slot, 0, k)
            sums[k] = part
        finish(slot, (2,))
        for k in range(total):
            part = sums[k] + faces_z[2, k] * halo_up_z(slot, k)
            sums[k] = part + faces_z[3, k] * halo_down_z(slot, k)
        for x in range(planes):
            first, second = sums[x], sums[x] + sums[planes + x]
            if restart:
                basis[index + 1, x] = 0.5 * first
                basis[index + 1, planes + x] = 0.5 * second
            else:
                basis[index + 1, x] = first - basis[index - 1, x]
                basis[index + 1, planes + x] = second - basis[index - 1, planes + x]

    def sum_copy(which, target):
        return pltpu.make_async_remote_copy(
            src_ref=parts.at[which, pl.ds(me, 1)],
            dst_ref=parts.at[which, pl.ds(me, 1)],
            send_sem=sum_send.at[which],
            recv_sem=sum_recv.at[which],
            device_id=target,
            device_id_type=MESH,
        )

    def start_sum(which):
        ones = jnp.ones((8, lanes), jnp.float32)
        local = lax.dot_general(
            ones, gram[...], (((1,), (1,)), ((), ())), precision=highest,
            preferred_element_type=jnp.float32,
        )
        parts[which, pl.ds(me, 1), :] = local[0:1]
        if devices <= 64:
            for number in range(1, devices):
                dx, dy, dz = number // (ny * nz), number // nz % ny, number % nz
                target = tuple(
                    (place[d] + step) % sizes[d] if step else place[d]
                    for d, step in enumerate((dx, dy, dz))
                )
                sum_copy(which, target).start()
        else:

            def send(number, carry):
                other = (me + number) % devices
                sum_copy(which, (other // (ny * nz), other // nz % ny, other % nz)).start()
                return carry

            lax.fori_loop(1, devices, send, 0)
    def finish_sum(which):
        everything = pltpu.make_async_remote_copy(
            src_ref=parts.at[which, pl.ds(0, devices - 1)],
            dst_ref=parts.at[which, pl.ds(0, devices - 1)],
            send_sem=sum_send.at[which],
            recv_sem=sum_recv.at[which],
            device_id=((place[0] + 1) % nx, place[1], place[2]),
            device_id_type=MESH,
        )
        everything.wait_recv()
        pending.append(everything)
        summed = jnp.broadcast_to(
            jnp.sum(parts[which], axis=0, keepdims=True), (rows, lanes)
        )

        def entry(number):
            return jnp.broadcast_to(summed[:, number : number + 1], (rows, lanes))

        return entry

    def triangle(j):
        return j * (j + 1) // 2

    for j in range(FIRST):
        advance((j + 1) % 2, j, j == 0, lambda j=j: dots(j, range(j + 1), triangle(j)))
    dots(FIRST, range(FIRST), triangle(FIRST))
    start_sum(0)
    found = {}
    pending = []

    def orthonormalise():
        entry = finish_sum(0)
        matrix = {}
        for j in range(FIRST):
            for i in range(j, FIRST):
                matrix[i, j] = entry(triangle(i) + j)
        factors = cholesky(matrix, FIRST)
        on_ortho = forward_solve(*factors, [entry(triangle(FIRST) + i) for i in range(FIRST)])
        shares = backward_solve(*factors, on_ortho)
        at_one = forward_solve(*factors, [jnp.ones((rows, lanes), jnp.float32)] * FIRST)
        last = 1.0 - on_ortho[0] * at_one[0]
        for i in range(1, FIRST):
            last = last - on_ortho[i] * at_one[i]
        found.update(
            factors=factors, shares=shares, at_one=at_one + [last] * (KRYLOV + 1 - FIRST)
        )
        lower, inverse_diag = factors
        for k in range(total):
            made = []
            for i in range(FIRST):
                value = basis[i, k]
                for m in range(i):
                    value = value - lower[i, m] * made[m]
                value = value * inverse_diag[i]
                made.append(value)
                basis[ORTHO + i, k] = value
        for i in range(FIRST):
            dots(ORTHO + i, range(ORTHO, ORTHO + i + 1), triangle(i))

    for j in range(FIRST, FIRST + LAG):
        advance(
            (j + 1) % 2, j, False, orthonormalise if j == FIRST + LAG - 1 else lambda: None
        )
    shares = found["shares"]
    pending.pop().wait_send()

    middle = ORTHO + FIRST
    for k in range(total):
        value = basis[FIRST, k]
        for i in range(FIRST):
            value = value - shares[i] * basis[i, k]
        basis[middle, k] = value
        for m in range(1, LAG + 1):
            value = basis[FIRST + m, k] + basis[abs(FIRST - m), k]
            for i in range(FIRST):
                value = value - shares[i] * (basis[i + m, k] + basis[abs(i - m), k])
            basis[middle + m, k] = 0.5 * value
    for j in range(FIRST + LAG, KRYLOV):

        def between(j=j):
            for i in range(FIRST if j == FIRST + LAG else j, j + 1):
                dots(ORTHO + i, range(ORTHO, ORTHO + i + 1), triangle(i))

        advance((j + 1) % 2, ORTHO + j, False, between)
    dots(ORTHO + KRYLOV, range(ORTHO, ORTHO + KRYLOV + 1), triangle(KRYLOV))
    start_sum(1)
    drain(KRYLOV % 2)
    entry = finish_sum(1)
    matrix = {}
    for i in range(KRYLOV + 1):
        for j in range(i + 1):
            matrix[i, j] = entry(triangle(i) + j)
    factors = cholesky(matrix, KRYLOV + 1)
    half = forward_solve(*factors, found["at_one"])
    length = half[0] * half[0]
    for value in half[1:]:
        length = length + value * value
    weights = backward_solve(*factors, [value / length for value in half])

    target = backward_solve(*found["factors"], weights[:FIRST]) + weights[FIRST:]
    z = [None] * KRYLOV
    for i in range(KRYLOV, 0, -1):
        value = target[i] + z[i] if i < KRYLOV else target[i]
        above = z[i + 1] if i + 1 < KRYLOV and i != FIRST - 1 else None
        if i < FIRST:
            share = shares[i] * z[FIRST - 1]
            above = share if above is None else above + share
        if i in (1, FIRST + 1):
            z[i - 1] = value - 0.5 * above
        else:
            z[i - 1] = 2.0 * value if above is None else 2.0 * value - above

    for x in range(planes):
        first = z[0] * basis[0, x]
        second = z[0] * basis[0, planes + x]
        for j in range(1, KRYLOV):
            at = j if j < FIRST else ORTHO + j
            first = first + z[j] * basis[at, x]
            second = second + z[j] * basis[at, planes + x]
        solution_ref[0, x] = inverse[0, x] * first + inverse[1, x] * second
        solution_ref[1, x] = inverse[1, x] * first + inverse[2, x] * second
    for k, (c, x) in enumerate(order):
        value = weights[0] * basis[ORTHO, k]
        for j in range(1, KRYLOV + 1):
            value = value + weights[j] * basis[ORTHO + j, k]
        residual_ref[c, x] = value
    pending.pop().wait_send()


def solution(mesh):
    sizes = tuple(mesh.shape[axis] for axis in AXES)
    devices = sizes[0] * sizes[1] * sizes[2]

    def body(source, sigma_intra, sigma_extra, membrane):
        planes, rows, lanes = membrane.shape
        total = 2 * planes
        f32 = jnp.float32
        vmem = pl.BlockSpec(memory_space=pltpu.VMEM)
        return pl.pallas_call(
            functools.partial(kernel, sizes),
            out_shape=(jax.ShapeDtypeStruct(source.shape, f32),) * 2,
            in_specs=[pl.BlockSpec(memory_space=pl.ANY)] * 4,
            out_specs=(vmem, vmem),
            scratch_shapes=[
                pltpu.VMEM((ORTHO + KRYLOV + 1, total, rows, lanes), f32),
                pltpu.VMEM((2, total, rows, lanes), f32),
                pltpu.VMEM((4, total, rows, lanes), f32),
                pltpu.VMEM((4, total, rows, lanes), f32),
                pltpu.VMEM((3, planes, rows, lanes), f32),
                pltpu.VMEM((2, 2, planes, rows, lanes), f32),
                pltpu.VMEM((2, 2, total, lanes), f32),
                pltpu.VMEM((2, rows, lanes), f32),
                pltpu.VMEM((2, 2, 2, rows, lanes), f32),
                pltpu.VMEM((2, 2, total, lanes), f32),
                pltpu.VMEM((2, 2, rows, lanes), f32),
                pltpu.VMEM((128, lanes), f32),
                pltpu.VMEM((2, devices, 128), f32),
                pltpu.SemaphoreType.DMA((2, 3, 2)),
                pltpu.SemaphoreType.DMA((2, 3, 2)),
                pltpu.SemaphoreType.DMA((2,)),
                pltpu.SemaphoreType.DMA((2,)),
                pltpu.VMEM(sigma_intra.shape, f32),
                pltpu.VMEM(sigma_extra.shape, f32),
                pltpu.VMEM(membrane.shape, f32),
                pltpu.SemaphoreType.DMA((4,)),
            ],
            compiler_params=pltpu.CompilerParams(collective_id=0, has_side_effects=True),
        )(source.reshape(total, rows, lanes), sigma_intra, sigma_extra, membrane)

    spec = P(None, "gx", "gy", "gz")
    return jax.shard_map(
        body,
        mesh=mesh,
        in_specs=(spec, spec, spec, P("gx", "gy", "gz")),
        out_specs=(spec, spec),
        check_vma=False,
    )
```
